256 devices in a mesh: comp: 32 (over z_lo, x, core), rows: 8 (over y, z_hi).
Axes of the slice: x: 4, y: 4, z: 8 (z_hi: 2, z_lo: 4; z = z_hi * 4 + z_lo), core: 2. Of those that a mesh axis runs over, the one named last changes fastest.
Arguments:
- hidden_states: bfloat16 [8, 2, 32, 128, 2560], P('rows', None, 'comp'), may hold values from -6 to 6
- queries: bfloat16 [8, 2, 32, 128, 1280], P('rows', None, 'comp'), may hold values from -900 to 900
- new_keys: bfloat16 [8, 2, 32, 128, 1280], P('rows', None, 'comp'), may hold values from -6 to 6
- new_values: bfloat16 [8, 2, 32, 128, 1280], P('rows', None, 'comp'), may hold values from -6 to 6
- out_grad: bfloat16 [8, 2, 32, 128, 1280], P('rows', None, 'comp'), may hold values from -6 to 6
- gate_weight: bfloat16 [2560, 128], replicated, may hold values from -0.125 to 0.125
- gate_bias: float32 [128], replicated, may hold values from -2 to 6
- prompt_state: float32 [8, 32, 2, 2, 2, 64, 640], P('rows', 'comp'), may hold values from -6 to 6
- owners: int32 [8, 2], P('rows'), may hold values from 0 to 31
- lengths: int32 [8, 2, 32], P('rows', None, 'comp'), may hold values from 32 to 128
- advantage: float32 [8, 2, 32], P('rows', None, 'comp'), may hold values from -4 to 4
Outputs:
- d_queries: bfloat16 [8, 2, 32, 128, 1280], P('rows', None, 'comp')
- d_keys: bfloat16 [8, 2, 32, 128, 1280], P('rows', None, 'comp')
- d_values: bfloat16 [8, 2, 32, 128, 1280], P('rows', None, 'comp')
- d_hidden: bfloat16 [8, 2, 32, 128, 2560], P('rows', None, 'comp')
- d_gate_weight: float32 [2560, 128], replicated
- d_gate_bias: float32 [128], replicated
- d_state: float32 [8, 2, 2, 2, 64, 640], P('rows', None, None, None, 'comp')
The draws below stay inside these ranges and needn't reach their ends.
All inputs are finite; a program needn't handle non-finite values.
Results may differ from the reference program's by a relative error of at most 0.011.
Values sent between devices are 32-bit elements; how exact they have to be, the bound alone decides.
No kernel may reach another device: no remote copies, remote signals or barrier semaphores. Data moves between devices by JAX's collectives and lax.ppermute only.
A program may use at most 64 MiB of HBM per device.

```python
import jax
import jax.numpy as jnp
from jax import lax

D = 2560
H = 2
DH = 640
M = 64
LEN = 128
PR_ROW = 2
COMPS = 32
N_COMP = 32
N_ROWS = 8


def draw_queries(key, part):
    shape = (N_ROWS, PR_ROW, COMPS, LEN, H * DH)
    values = jnp.clip(jax.random.normal(key, shape, jnp.float32), -6.0, 6.0)
    return values.astype(jnp.bfloat16)


def plant(drawn, rng, low, largest):
    spot = [jax.random.randint(jax.random.fold_in(rng, axis), (), 0, length) for axis, length in enumerate(drawn.shape)]
    main_axis = drawn.shape.index(max(drawn.shape))
    beside = spot[:main_axis] + [(spot[main_axis] + 1) % drawn.shape[main_axis]] + spot[main_axis + 1:]
    return drawn.at[tuple(spot)].set(low).at[tuple(beside)].set(largest)


def block_levels(own_key, dims, pieces, low, largest):
    level, own = 1.0, jax.random.fold_in(own_key, 6)
    for dim, blocks in pieces:
        draws = jnp.exp(jax.random.uniform(jax.random.fold_in(own, dim), (blocks,), jnp.float32, low / len(pieces), largest / len(pieces)))
        level = level * jnp.repeat(draws, dims[dim] // blocks).reshape([-1 if axis == dim else 1 for axis in range(len(dims))])
    return level


def noise(rng, extent, scale, limit, split=(), kind=jnp.bfloat16):
    array = scale * jax.random.normal(rng, extent, jnp.float32)
    if split:
        array = array * block_levels(rng, extent, split, -0.22, 0.18)
    return jnp.clip(array, -limit, limit).astype(kind)


def setup_inputs(seed: int = 0) -> dict:
    arg_keys = jax.random.split(jax.random.key(seed), 12)
    hidden_states = noise(arg_keys[0], (N_ROWS, PR_ROW, COMPS, LEN, D), 1.0, 6.0, ((0, 8), (2, 32)))
    queries = draw_queries(jax.random.fold_in(arg_keys[11], 71), 0)
    new_keys = noise(arg_keys[2], (N_ROWS, PR_ROW, COMPS, LEN, H * DH), 1.0, 6.0, ((0, 8), (2, 32)))
    new_values = noise(arg_keys[3], (N_ROWS, PR_ROW, COMPS, LEN, H * DH), 1.0, 6.0, ((0, 8), (2, 32)))
    out_grad = noise(arg_keys[4], (N_ROWS, PR_ROW, COMPS, LEN, H * DH), 1.0, 6.0, ((0, 8), (2, 32)))
    gate_weight = noise(arg_keys[5], (D, H * M), D ** -0.5, 0.125)
    gate_bias = jnp.clip(jax.random.uniform(arg_keys[6], (H * M,), jnp.float32, -2.0, 6.0), -2.0, 6.0)
    prompt_state = noise(arg_keys[7], (N_ROWS, N_COMP, PR_ROW, 2, H, M, DH), 1.0, 6.0, ((0, 8), (1, 32)), jnp.float32)
    owners = plant(jax.random.randint(arg_keys[8], (N_ROWS, PR_ROW), 0, N_COMP), jax.random.fold_in(arg_keys[8], 1), 0, N_COMP - 1).astype(jnp.int32)
    lengths = plant(jax.random.randint(arg_keys[9], (N_ROWS, PR_ROW, COMPS), LEN // 4, LEN + 1), jax.random.fold_in(arg_keys[9], 1), LEN // 4, LEN).astype(jnp.int32)
    advantage = noise(arg_keys[10], (N_ROWS, PR_ROW, COMPS), 1.0, 4.0, ((0, 8), (2, 32)), jnp.float32)
    return {"hidden_states": hidden_states, "queries": queries, "new_keys": new_keys, "new_values": new_values, "out_grad": out_grad, "gate_weight": gate_weight, "gate_bias": gate_bias, "prompt_state": prompt_state, "owners": owners, "lengths": lengths, "advantage": advantage}


def slot_forward(gates, queries, keys_in, values_in, anchor_point):
    steps = queries.shape[0]
    heads = anchor_point.shape[1]
    slots = anchor_point.shape[2]
    width = anchor_point.shape[3]
    highest_score = lax.Precision.HIGHEST
    log_keep = jax.nn.log_sigmoid(gates).reshape(steps, heads, slots) / 8.0
    running = jnp.cumsum(log_keep, axis=0)
    inflow = -jnp.expm1(log_keep)
    places = jnp.arange(steps, dtype=jnp.int32)
    lower = (places[:, None] >= places[None, :])[:, :, None, None]
    between = running[:, None] - running[None, :]
    reach = jnp.where(lower, jnp.exp(jnp.where(lower, between, 0.0)), 0.0) * inflow[None]
    score_scale = width ** (-0.5)
    query_head_count = queries.astype(jnp.float32).reshape(steps, heads, width)
    key_heads = keys_in.astype(jnp.float32).reshape(steps, heads, width)
    value_heads = values_in.astype(jnp.float32).reshape(steps, heads, width)
    pairs = jnp.einsum('thd,jhd->thj', query_head_count, key_heads) * score_scale
    carried_state = jnp.exp(running)
    anchor_score_rows = jnp.einsum('icv,crv->icr', query_head_count, anchor_point[0], precision=highest_score) * score_scale
    scores = jnp.einsum('tjhm,thj->thm', reach, pairs, precision=highest_score) + carried_state * anchor_score_rows
    slot_probabilities = jax.nn.softmax(scores, axis=-1)
    mixing = jnp.einsum('thm,tjhm->thj', slot_probabilities, reach, precision=highest_score).astype(jnp.bfloat16)
    result_output = jnp.einsum('thj,jhd->thd', mixing.astype(jnp.float32), value_heads)
    result_output = result_output + jnp.einsum('ivw,vwb->ivb', slot_probabilities * carried_state, anchor_point[1], precision=highest_score)
    return result_output.reshape(steps, heads * width)

def completion_grads(tokens, queries, keys_in, values_in, out_grad, gate_weight, gate_bias, anchor_point, length, advantage):
    steps = queries.shape[0]
    gates = jnp.dot(tokens, gate_weight, preferred_element_type=jnp.float32) + gate_bias
    places = jnp.arange(steps, dtype=jnp.int32)
    live = jnp.where(places < length, 1.0, 0.0).astype(jnp.float32)
    cotangent = (advantage * live)[:, None] * out_grad.astype(jnp.float32)
    result_output, pullback = jax.vjp(slot_forward, gates, queries, keys_in, values_in, anchor_point)
    grad_gates, grad_q, grad_k, grad_v, grad_anchor = pullback(cotangent)
    gates_low = grad_gates.astype(jnp.bfloat16)
    grad_tokens = jnp.dot(gates_low, gate_weight.T, preferred_element_type=jnp.float32).astype(jnp.bfloat16)
    grad_weight = jnp.dot(tokens.T, gates_low, preferred_element_type=jnp.float32)
    grad_bias = lax.optimization_barrier(jnp.sum(grad_gates, axis=0))
    return (grad_q.astype(jnp.bfloat16), grad_k.astype(jnp.bfloat16), grad_v.astype(jnp.bfloat16), grad_tokens, grad_weight, grad_bias, grad_anchor)

def reference(hidden_states, queries, new_keys, new_values, out_grad, gate_weight, gate_bias, prompt_state, owners, lengths, advantage):
    total = N_ROWS * PR_ROW * COMPS

    def visit(carry, index):
        sum_weight, sum_bias, sum_state = carry
        row = index // (PR_ROW * COMPS)
        prompt = index // COMPS % PR_ROW
        column = index % COMPS
        anchor_point = prompt_state[row, owners[row, prompt], prompt]
        grads = completion_grads(hidden_states[row, prompt, column], queries[row, prompt, column], new_keys[row, prompt, column], new_values[row, prompt, column], out_grad[row, prompt, column], gate_weight, gate_bias, anchor_point, lengths[row, prompt, column], advantage[row, prompt, column])
        sum_state = sum_state.at[row, prompt].add(grads[6])
        return ((sum_weight + grads[4], sum_bias + grads[5], sum_state), (grads[0], grads[1], grads[2], grads[3]))
    start = (jnp.zeros((D, H * M), jnp.float32), jnp.zeros((H * M,), jnp.float32), jnp.zeros((N_ROWS, PR_ROW, 2, H, M, DH), jnp.float32))
    (sum_weight, sum_bias, sum_state), stacked = lax.scan(visit, start, jnp.arange(total, dtype=jnp.int32))
    shape_heads = (N_ROWS, PR_ROW, COMPS, LEN, H * DH)
    d_queries = stacked[0].reshape(shape_heads)
    d_keys = stacked[1].reshape(shape_heads)
    d_values = stacked[2].reshape(shape_heads)
    d_hidden = stacked[3].reshape((N_ROWS, PR_ROW, COMPS, LEN, D))
    return (d_queries, d_keys, d_values, d_hidden, sum_weight, sum_bias, sum_state)
```

```python
import jax
import jax.numpy as jnp
from jax import lax
from jax.experimental import pallas as pl
from jax.experimental.pallas import tpu as pltpu
from jax.sharding import Mesh
from jax.sharding import PartitionSpec as P

F32 = jnp.float32
BF16 = jnp.bfloat16
D = 2560
T = 128
HM = 128
DH = 640
LEVELS = (64, 32, 16, 8, 4, 2, 1)
SCALE = DH ** (-0.5)
WROWS = 1280
BROWS = 8


def split2(x):
    high = x.astype(BF16)
    return high, (x - high.astype(F32)).astype(BF16)


def split3(x):
    high = x.astype(BF16)
    rest = x - high.astype(F32)
    middle = rest.astype(BF16)
    return high, middle, (rest - middle.astype(F32)).astype(BF16)


def mm(a, b):
    return jnp.dot(a, b, preferred_element_type=F32)


def mm_nt(a, b):
    return lax.dot_general(a, b, (((1,), (1,)), ((), ())), preferred_element_type=F32)


def mm_tn(a, b):
    return lax.dot_general(a, b, (((0,), (0,)), ((), ())), preferred_element_type=F32)


def mask_matmul(mask, x):
    high, middle, low = split3(x)
    return mm(mask, high) + mm(mask, middle) + mm(mask, low)


def iota(dim, shape):
    return lax.broadcasted_iota(jnp.int32, shape, dim)


def one_where(condition):
    return jnp.where(condition, 1.0, 0.0).astype(BF16)


def same_block(size, rows, cols):
    shift = size.bit_length() - 1
    row = jnp.right_shift(jnp.bitwise_and(iota(0, (rows, cols)), T - 1), shift)
    col = jnp.right_shift(jnp.bitwise_and(iota(1, (rows, cols)), T - 1), shift)
    return row == col


def odd_half(size):
    return jnp.bitwise_and(iota(0, (T, HM)), size) != 0


def pick_kernel(place, states, keep, send):
    core, x, z = place[0], place[1], place[2]
    for turn, out in ((0, keep), (1, send)):
        prompt = jnp.bitwise_xor(core, turn)
        owned = place[4 + prompt] == 1
        for kx in range(4):
            for kz in range(4):
                row = jnp.bitwise_xor(z, kz) * 16
                block = states[prompt, jnp.bitwise_xor(x, kx), pl.ds(pl.multiple_of(row, 16), 16), :]
                out[kx, kz] = jnp.where(owned, block, 0.0)


def first_kernel(place, adv, hid, q, k, v, og, wg, bias, vec, at, yz):
    prompt = pl.program_id(0)
    length = place[6 + prompt]
    weight = adv[prompt]
    gates = mm(hid[0], wg[...]) + bias[...]
    u = jnp.exp(-jnp.abs(gates))
    s = u / (2.0 + u)
    s2 = s * s
    series = 1.0 / 17.0
    for n in (15, 13, 11, 9, 7, 5, 3, 1):
        series = series * s2 + 1.0 / n
    log1p = 2.0 * s * series
    log_keep = (jnp.minimum(gates, 0.0) - log1p) * 0.125
    keep = jnp.exp(log_keep)
    near = 1.0 + log_keep * (1.0 / 8.0)
    for n in (7, 6, 5, 4, 3, 2):
        near = 1.0 + log_keep * (1.0 / n) * near
    inflow = jnp.where(log_keep > -0.3, -log_keep * near, 1.0 - keep)
    slope = jnp.where(gates >= 0.0, u, 1.0) / (1.0 + u) * 0.125
    row = iota(0, (T, T))
    col = iota(1, (T, T))
    running = mask_matmul(one_where(col <= row), log_keep)
    vec[0, 0] = jnp.exp(running)
    vec[0, 1] = inflow
    vec[0, 2] = keep
    vec[0, 3] = slope

    live_col = jnp.where(iota(0, (T, 1)) < length, weight, 0.0)
    live_row = jnp.where(iota(1, (1, T)) < length, weight, 0.0)
    pairs, grads = [], []
    for h in range(2):
        cols = slice(h * DH, (h + 1) * DH)
        qh, kh, vh, gh = q[0, :, cols], k[0, :, cols], v[0, :, cols], og[0, :, cols]
        pairs.append(mm_nt(qh, kh) * SCALE)
        grads.append(mm_nt(gh, vh) * live_col)
        at[0, h * T : (h + 1) * T, 0:T] = mm_nt(kh, qh) * SCALE
        at[0, h * T : (h + 1) * T, T : 2 * T] = mm_nt(vh, gh) * live_row
    pairs = jnp.concatenate(pairs, axis=1)
    grads = jnp.concatenate(grads, axis=1)
    head0 = iota(1, (T, HM)) < 64
    grads_high, grads_low = split2(grads)

    def level(y, z, block):
        zs = jnp.concatenate([jnp.where(head0, z, 0.0), jnp.where(head0, 0.0, z)], axis=0)
        zs_high, zs_low = split2(zs)
        same = same_block(block, T, 2 * T)
        score = jnp.dot(jnp.where(same, pairs, 0.0), zs, precision=lax.Precision.HIGHEST, preferred_element_type=F32)
        gh = jnp.where(same, grads_high.astype(F32), 0.0).astype(BF16)
        gl = jnp.where(same, grads_low.astype(F32), 0.0).astype(BF16)
        grad = mm(gh, zs_high) + mm(gl, zs_high) + mm(gh, zs_low)
        if y is None:
            return score, grad
        return y * score, y * grad

    s1, t1 = level(None, inflow, 1)
    for n, size in enumerate(LEVELS):
        start = jnp.bitwise_and(row, -size)
        odd = jnp.bitwise_and(row, size) != 0
        low = jnp.where(odd, start, row + 1)
        high = jnp.where(odd, row, start + size - 1)
        decay = jnp.exp(mask_matmul(one_where((col >= low) & (col <= high)), log_keep))
        yz[0, n] = decay
        odd = odd_half(size)
        score, grad = level(jnp.where(odd, decay, 0.0), jnp.where(odd, 0.0, decay * inflow), 2 * size)
        s1 = s1 + score
        t1 = t1 + grad
    vec[0, 4] = s1
    vec[0, 5] = t1


def second_kernel(place, adv, vec, at, yz, hid, q, og, mine, other, pd, dgl, kz_out, ds_keep, ds_send, dw_keep, dw_send, acc, bacc, kv):
    step = pl.program_id(0)
    core, x, z, y = place[0], place[1], place[2], place[3]
    prompt = jnp.bitwise_xor(step, core)
    length = place[6 + prompt]
    weight = adv[prompt]

    def gather(source):
        for i in range(4):
            for j in range(4):
                kv[i, j * 16 : (j + 1) * 16, :] = source[jnp.bitwise_xor(x, i), jnp.bitwise_xor(z, j)]

    @pl.when(step == 0)
    def _():
        gather(mine)

    @pl.when(step == 1)
    def _():
        gather(other)

    live_col = jnp.where(iota(0, (T, 1)) < length, weight, 0.0)
    carried = vec[0, 0]
    inflow = vec[0, 1]
    keep = vec[0, 2]
    slope = vec[0, 3]
    head0 = iota(1, (T, HM)) < 64
    anchor_score, anchor_grad = [], []
    for h in range(2):
        cols = slice(h * DH, (h + 1) * DH)
        qh, gh = q[0, :, cols], og[0, :, cols]
        a, b, c = split3(kv[h])
        kz_out[0, h * 64 : (h + 1) * 64, :] = a
        anchor_score.append(mm_nt(qh, a) + mm_nt(qh, b) + mm_nt(qh, c))
        a, b = split2(kv[2 + h])
        anchor_grad.append(mm_nt(gh, a) + mm_nt(gh, b))
    anchor_score = jnp.concatenate(anchor_score, axis=1) * SCALE
    anchor_grad = jnp.concatenate(anchor_grad, axis=1) * live_col
    scores = vec[0, 4] + carried * anchor_score
    top0 = jnp.max(jnp.where(head0, scores, -jnp.inf), axis=1, keepdims=True)
    top1 = jnp.max(jnp.where(head0, -jnp.inf, scores), axis=1, keepdims=True)
    e = jnp.exp(scores - jnp.where(head0, top0, top1))
    sum0 = jnp.sum(jnp.where(head0, e, 0.0), axis=1, keepdims=True)
    sum1 = jnp.sum(jnp.where(head0, 0.0, e), axis=1, keepdims=True)
    probs = e / jnp.where(head0, sum0, sum1)
    d_probs = vec[0, 5] + carried * anchor_grad
    weighted = probs * d_probs
    dot0 = jnp.sum(jnp.where(head0, weighted, 0.0), axis=1, keepdims=True)
    dot1 = jnp.sum(jnp.where(head0, 0.0, weighted), axis=1, keepdims=True)
    d_scores = probs * (d_probs - jnp.where(head0, dot0, dot1))
    pd[0, 0] = probs
    pd[0, 1] = d_scores

    order = iota(0, (HM, HM))
    slot = iota(1, (HM, HM))
    place_c = jnp.bitwise_xor(jnp.bitwise_and(jnp.right_shift(order, 5), 1), core)
    place_x = jnp.bitwise_xor(jnp.bitwise_and(jnp.right_shift(order, 3), 3), x)
    place_z = jnp.bitwise_xor(jnp.bitwise_and(jnp.right_shift(order, 1), 3), z)
    wanted = jnp.bitwise_and(order, 64) + place_z * 16 + place_x * 4 + place_c * 2 + jnp.bitwise_and(order, 1)
    move = one_where(slot == wanted)
    d_anchor = d_scores * carried * SCALE
    for kind, (term, rows) in enumerate(((d_anchor, q), (probs * carried * live_col, og))):
        high, low = split2(term)
        high = mm_nt(move, high).astype(BF16)
        low = mm_nt(move, low).astype(BF16)
        for h in range(2):
            data = rows[0, :, h * DH : (h + 1) * DH]
            part = slice(h * 64, (h + 1) * 64)
            total = mm(high[part], data) + mm(low[part], data)
            for kx in range(4):
                ds_keep[kx, 0, kind, h] = total[kx * 8 : kx * 8 + 8]
                ds_send[kx, 0, kind, h] = total[32 + kx * 8 : 32 + kx * 8 + 8]

    at_high, at_low = split2(at[0])
    at_high, at_low = at_high.astype(F32), at_low.astype(F32)

    def level(left, block):
        high, low = split2(left)
        same = same_block(block, 2 * T, 2 * T)
        ah = jnp.where(same, at_high, 0.0).astype(BF16)
        al = jnp.where(same, at_low, 0.0).astype(BF16)
        out = mm(ah, high) + mm(al, high) + mm(ah, low)
        return jnp.where(head0, out[0:T], out[T : 2 * T])

    both = jnp.concatenate([d_scores, probs], axis=0)
    held = level(both, 1)
    for n, size in enumerate(LEVELS):
        decay = yz[0, n]
        odd = odd_half(size)
        later = jnp.where(odd, decay, 0.0)
        earlier = jnp.where(odd, 0.0, decay)
        held = held + earlier * level(both * jnp.concatenate([later, later], axis=0), 2 * size)
    change = d_scores * scores + probs * d_probs - held * inflow
    row = iota(0, (T, T))
    col = iota(1, (T, T))
    d_log_keep = mask_matmul(one_where(col >= row), change) - held * keep
    d_gates = d_log_keep * slope
    low_gates = d_gates.astype(BF16)
    dgl[0] = low_gates
    bias = jnp.sum(d_gates, axis=0, keepdims=True)

    @pl.when(step == 0)
    def _():
        acc[...] = mm_tn(hid[0], low_gates)
        bacc[...] = jnp.broadcast_to(bias, (BROWS, HM))

    @pl.when(step == 1)
    def _():
        acc[...] = acc[...] + mm_tn(hid[0], low_gates)
        total = bacc[...] + bias
        for kc, out in ((0, dw_keep), (1, dw_send)):
            out[WROWS : WROWS + BROWS, :] = total
            for ky in range(4):
                for kx in range(4):
                    block = jnp.bitwise_xor(core, kc) * 16 + jnp.bitwise_xor(y, ky) * 4 + jnp.bitwise_xor(x, kx)
                    start = (ky * 4 + kx) * 80
                    out[start : start + 80, :] = acc[pl.ds(pl.multiple_of(block * 80, 8), 80), :]


def third_kernel(place, adv, vec, yz, pd, dgl, k0, q, k, og, wg, dq, dk, dv, dx):
    prompt = pl.program_id(0)
    length = place[6 + prompt]
    weight = adv[prompt]
    live_col = jnp.where(iota(0, (T, 1)) < length, weight, 0.0)
    dx[0] = mm_nt(dgl[0], wg[...]).astype(BF16)
    inflow = vec[0, 1]
    probs = pd[0, 0]
    d_scores = pd[0, 1]
    head0 = iota(1, (T, HM)) < 64
    both = jnp.concatenate([probs, d_scores], axis=0)

    def level(left, right, block):
        zs = jnp.concatenate([jnp.where(head0, right, 0.0), jnp.where(head0, 0.0, right)], axis=0)
        zh, zl = split2(zs)
        lh, ll = split2(left)
        out = mm_nt(lh, zh) + mm_nt(ll, zh) + mm_nt(lh, zl)
        return jnp.where(same_block(block, 2 * T, 2 * T), out, 0.0)

    mix = level(both, inflow, 1)
    for n, size in enumerate(LEVELS):
        decay = yz[0, n]
        odd = odd_half(size)
        later = jnp.where(odd, decay, 0.0)
        earlier = jnp.where(odd, 0.0, decay * inflow)
        mix = mix + level(both * jnp.concatenate([later, later], axis=0), earlier, 2 * size)
    d_anchor = (d_scores * vec[0, 0]).astype(BF16)
    for h in range(2):
        cols = slice(h * DH, (h + 1) * DH)
        qh, kh, gh = q[0, :, cols], k[0, :, cols], og[0, :, cols]
        mixing = mix[0:T, h * T : (h + 1) * T].astype(BF16).astype(F32)
        d_pairs = mix[T : 2 * T, h * T : (h + 1) * T].astype(BF16)
        from_anchor = mm(d_anchor[:, h * 64 : (h + 1) * 64], k0[0, h * 64 : (h + 1) * 64, :])
        dq[0, :, cols] = ((mm(d_pairs, kh) + from_anchor) * SCALE).astype(BF16)
        dk[0, :, cols] = (mm_tn(d_pairs, qh) * SCALE).astype(BF16)
        dv[0, :, cols] = mm_tn((mixing * live_col).astype(BF16), gh).astype(BF16)


def place_kernel(place, mine, other, out):
    core, x, y = place[0], place[1], place[3]
    for kc, source in ((0, mine), (1, other)):
        for ky in range(4):
            for kx in range(4):
                block = jnp.bitwise_xor(core, kc) * 16 + jnp.bitwise_xor(y, ky) * 4 + jnp.bitwise_xor(x, kx)
                out[pl.ds(pl.multiple_of(block * 80, 8), 80), :] = source[ky, kx]


SMEM = pltpu.SMEM
VMEM = pltpu.VMEM


def whole(memory=VMEM):
    return pl.BlockSpec(memory_space=memory)


def fixed(shape):
    return pl.BlockSpec(shape, lambda i, *_: (0,) * len(shape))


def per_prompt(shape):
    return pl.BlockSpec((1,) + shape, lambda i, *_: (i,) + (0,) * len(shape))


def own_first(shape):
    return pl.BlockSpec((1,) + shape, lambda i, place, *_: (jnp.bitwise_xor(i, place[0]),) + (0,) * len(shape))


def swap(value, axis, mask):
    count = 1
    for name in axis if isinstance(axis, tuple) else (axis,):
        count *= lax.axis_size(name)
    return lax.ppermute(value, axis, [(i, i ^ mask) for i in range(count)])


def tree_sum(parts):
    while len(parts) > 1:
        parts = [parts[i] + parts[i + 1] for i in range(0, len(parts), 2)]
    return parts[0]


def struct(shape, dtype=F32):
    return jax.ShapeDtypeStruct(shape, dtype)


def shards(hid, q, k, v, og, wg, bias, prompt_state, owners, lengths, advantage):
    hid, q, k, v, og = (a.reshape(2, T, a.shape[-1]) for a in (hid, q, k, v, og))
    states = prompt_state.reshape(2, 4, 64, DH)
    core, x, z, y = (lax.axis_index(n) for n in ("c", "x", "z", "y"))
    index = (z * 4 + x) * 2 + core
    mine = (owners.reshape(2) == index).astype(jnp.int32)
    place = jnp.concatenate([jnp.stack([core, x, z, y]).astype(jnp.int32), mine, lengths.reshape(2)])
    adv = advantage.reshape(2)

    with jax.named_scope("pick"):
        keep, send = pl.pallas_call(
            pick_kernel,
            out_shape=(struct((4, 4, 16, DH)), struct((4, 4, 16, DH))),
            in_specs=[whole(SMEM), whole()],
            out_specs=(whole(), whole()),
            name="pick",
        )(place, states)

    with jax.named_scope("anchors"):
        held = keep + swap(send, "c", 1)
        held = tree_sum([held[0]] + [swap(held[i], "x", i) for i in (1, 2, 3)])
        piece = tree_sum([held[0]] + [swap(held[i], "z", i) for i in (1, 2, 3)])
        column = jnp.stack([piece] + [swap(piece, "z", i) for i in (1, 2, 3)])
        mine = jnp.stack([column] + [swap(column, "x", i) for i in (1, 2, 3)])
        other = swap(mine, "c", 1)

    with jax.named_scope("first"):
        vec, at, yz = pl.pallas_call(
            first_kernel,
            grid_spec=pltpu.PrefetchScalarGridSpec(
                num_scalar_prefetch=2,
                grid=(2,),
                in_specs=[per_prompt((T, D))] + [per_prompt((T, 2 * DH))] * 4 + [fixed((D, HM)), fixed((1, HM))],
                out_specs=(per_prompt((6, T, HM)), per_prompt((2 * T, 2 * T)), per_prompt((7, T, HM))),
            ),
            out_shape=(struct((2, 6, T, HM)), struct((2, 2 * T, 2 * T)), struct((2, 7, T, HM))),
            cost_estimate=pl.CostEstimate(flops=int(6e9), bytes_accessed=int(6e6), transcendentals=0),
            name="first",
        )(place, adv, hid, q, k, v, og, wg, bias.reshape(1, HM))

    with jax.named_scope("second"):
        pd, dgl, k0, ds_keep, ds_send, dw_keep, dw_send = pl.pallas_call(
            second_kernel,
            grid_spec=pltpu.PrefetchScalarGridSpec(
                num_scalar_prefetch=2,
                grid=(2,),
                in_specs=[
                    own_first((6, T, HM)),
                    own_first((2 * T, 2 * T)),
                    own_first((7, T, HM)),
                    own_first((T, D)),
                    own_first((T, 2 * DH)),
                    own_first((T, 2 * DH)),
                    fixed((4, 4, 16, DH)),
                    fixed((4, 4, 16, DH)),
                ],
                out_specs=(
                    own_first((2, T, HM)),
                    own_first((T, HM)),
                    own_first((HM, DH)),
                    pl.BlockSpec((4, 1, 2, 2, 8, DH), lambda i, p, *_: (0, jnp.bitwise_xor(i, p[0]), 0, 0, 0, 0)),
                    pl.BlockSpec((4, 1, 2, 2, 8, DH), lambda i, p, *_: (0, jnp.bitwise_xor(i, p[0]), 0, 0, 0, 0)),
                    fixed((WROWS + BROWS, HM)),
                    fixed((WROWS + BROWS, HM)),
                ),
                scratch_shapes=[VMEM((D, HM), F32), VMEM((BROWS, HM), F32), VMEM((4, 64, DH), F32)],
            ),
            out_shape=(
                struct((2, 2, T, HM)),
                struct((2, T, HM), BF16),
                struct((2, HM, DH), BF16),
                struct((4, 2, 2, 2, 8, DH)),
                struct((4, 2, 2, 2, 8, DH)),
                struct((WROWS + BROWS, HM)),
                struct((WROWS + BROWS, HM)),
            ),
            cost_estimate=pl.CostEstimate(flops=int(6e9), bytes_accessed=int(10e6), transcendentals=0),
            name="second",
        )(place, adv, vec, at, yz, hid, q, og, mine, other)

    with jax.named_scope("weight"):
        held = dw_keep + swap(dw_send, "c", 1)
        for axis, rows in (("y", 320), ("x", 80)):
            tail = held[4 * rows :]
            parts = [jnp.concatenate([held[i * rows : (i + 1) * rows], tail]) for i in range(4)]
            held = tree_sum([parts[0]] + [swap(parts[i], axis, i) for i in (1, 2, 3)])
        held = tree_sum([held] + [swap(held, ("z", "zh"), i) for i in range(1, 8)])
        d_bias = held[80]
        piece = held[:80]
        line = jnp.stack([piece] + [swap(piece, "x", i) for i in (1, 2, 3)])
        mine = jnp.stack([line] + [swap(line, "y", i) for i in (1, 2, 3)])
        other = swap(mine, "c", 1)

    with jax.named_scope("state"):
        held = ds_keep + swap(ds_send, "c", 1)
        held = tree_sum([held[0]] + [swap(held[i], "x", i) for i in (1, 2, 3)])
        parts = [held[:, :, :, 2 * i : 2 * i + 2] for i in range(4)]
        d_state = tree_sum([parts[0]] + [swap(parts[i], "z", i) for i in (1, 2, 3)])

    with jax.named_scope("third"):
        dq, dk, dv, dx = pl.pallas_call(
            third_kernel,
            grid_spec=pltpu.PrefetchScalarGridSpec(
                num_scalar_prefetch=2,
                grid=(2,),
                in_specs=[
                    per_prompt((6, T, HM)),
                    per_prompt((7, T, HM)),
                    per_prompt((2, T, HM)),
                    per_prompt((T, HM)),
                    per_prompt((HM, DH)),
                    per_prompt((T, 2 * DH)),
                    per_prompt((T, 2 * DH)),
                    per_prompt((T, 2 * DH)),
                    fixed((D, HM)),
                ],
                out_specs=(per_prompt((T, 2 * DH)),) * 3 + (per_prompt((T, D)),),
            ),
            out_shape=(struct((2, T, 2 * DH), BF16),) * 3 + (struct((2, T, D), BF16),),
            cost_estimate=pl.CostEstimate(flops=int(6e9), bytes_accessed=int(8e6), transcendentals=0),
            name="third",
        )(place, adv, vec, yz, pd, dgl, k0, q, k, og, wg)

    with jax.named_scope("place"):
        d_weight = pl.pallas_call(
            place_kernel,
            out_shape=struct((D, HM)),
            in_specs=[whole(SMEM), whole(), whole()],
            out_specs=whole(),
            name="place",
        )(place, mine, other)

    def outer(a):
        return a.reshape(1, 2, 1, T, a.shape[-1])

    return outer(dq), outer(dk), outer(dv), outer(dx), d_weight, d_bias, d_state[None]


def solution(mesh):
    fine = Mesh(mesh.devices.reshape(4, 4, 2, 4, 2), ("z", "x", "c", "y", "zh"))
    comp = ("z", "x", "c")
    rows = ("y", "zh")
    tokens = P(rows, None, comp, None, None)
    return jax.shard_map(
        shards,
        mesh=fine,
        in_specs=(tokens,) * 5
        + (P(), P(), P(rows, comp, None, None, None, None, None), P(rows, None), P(rows, None, comp), P(rows, None, comp)),
        out_specs=(tokens,) * 4 + (P(), P(), P(rows, None, None, None, comp, None)),
        check_vma=False,
    )
```

```python
import functools

import jax
import jax.numpy as jnp
from jax import lax
from jax.experimental import pallas as pl
from jax.experimental.pallas import tpu as pltpu
from jax.sharding import Mesh
from jax.sharding import PartitionSpec as P


F32 = jnp.float32
BF16 = jnp.bfloat16
D = 2560
T = 128
HM = 128
DH = 640
LEVELS = (64, 32, 16, 8, 4, 2, 1)
SCALE = DH ** (-0.5)
WROWS = 1280
BROWS = 8


def split2(x):
    high = x.astype(BF16)
    return high, (x - high.astype(F32)).astype(BF16)


def split3(x):
    high = x.astype(BF16)
    rest = x - high.astype(F32)
    middle = rest.astype(BF16)
    return high, middle, (rest - middle.astype(F32)).astype(BF16)


def mm(a, b):
    return jnp.dot(a, b, preferred_element_type=F32)


def mm_nt(a, b):
    return lax.dot_general(a, b, (((1,), (1,)), ((), ())), preferred_element_type=F32)


def mm_tn(a, b):
    return lax.dot_general(a, b, (((0,), (0,)), ((), ())), preferred_element_type=F32)


def mask_matmul(mask, x):
    high, middle, low = split3(x)
    return mm(mask, high) + mm(mask, middle) + mm(mask, low)


def iota(dim, shape):
    return lax.broadcasted_iota(jnp.int32, shape, dim)


def one_where(condition):
    return jnp.where(condition, 1.0, 0.0).astype(BF16)


def same_block(size, rows, cols):
    shift = size.bit_length() - 1
    row = jnp.right_shift(jnp.bitwise_and(iota(0, (rows, cols)), T - 1), shift)
    col = jnp.right_shift(jnp.bitwise_and(iota(1, (rows, cols)), T - 1), shift)
    return row == col


def odd_half(size):
    return jnp.bitwise_and(iota(0, (T, HM)), size) != 0


def pick_kernel(owners, states, keep, send, buffer, sems):
    core, x, z = lax.axis_index("c"), lax.axis_index("x"), lax.axis_index("z")
    index = (z * 4 + x) * 2 + core
    copies = [
        pltpu.make_async_copy(states.at[jnp.bitwise_xor(core, turn)], buffer.at[turn], sems.at[turn])
        for turn in (0, 1)
    ]
    copies[1].start()
    copies[0].start()
    for turn, out in ((1, send), (0, keep)):
        owned = owners[0, jnp.bitwise_xor(core, turn)] == index
        copies[turn].wait()
        for kx in range(4):
            for kz in range(4):
                row = jnp.bitwise_xor(z, kz) * 16
                block = buffer[turn, jnp.bitwise_xor(x, kx), pl.ds(pl.multiple_of(row, 16), 16), :]
                out[kx, kz] = jnp.where(owned, block, 0.0)


def first_kernel(turn, place, adv, hid, q, k, v, og, wg, bias, vec, at, yz):
    prompt = jnp.bitwise_xor(place[0], turn)
    length = place[6 + prompt]
    weight = adv[prompt]
    gates = mm(hid[0], wg[...]) + bias[...]
    u = jnp.exp(-jnp.abs(gates))
    s = u / (2.0 + u)
    s2 = s * s
    series = 1.0 / 17.0
    for n in (15, 13, 11, 9, 7, 5, 3, 1):
        series = series * s2 + 1.0 / n
    log1p = 2.0 * s * series
    log_keep = (jnp.minimum(gates, 0.0) - log1p) * 0.125
    keep = jnp.exp(log_keep)
    near = 1.0 + log_keep * (1.0 / 8.0)
    for n in (7, 6, 5, 4, 3, 2):
        near = 1.0 + log_keep * (1.0 / n) * near
    inflow = jnp.where(log_keep > -0.3, -log_keep * near, 1.0 - keep)
    slope = jnp.where(gates >= 0.0, u, 1.0) / (1.0 + u) * 0.125
    row = iota(0, (T, T))
    col = iota(1, (T, T))
    running = mask_matmul(one_where(col <= row), log_keep)
    vec[0, 0] = jnp.exp(running)
    vec[0, 1] = inflow
    vec[0, 2] = keep
    vec[0, 3] = slope

    live_col = jnp.where(iota(0, (T, 1)) < length, weight, 0.0)
    live_row = jnp.where(iota(1, (1, T)) < length, weight, 0.0)
    pairs, grads = [], []
    for h in range(2):
        cols = slice(h * DH, (h + 1) * DH)
        qh, kh, vh, gh = q[0, :, cols], k[0, :, cols], v[0, :, cols], og[0, :, cols]
        pairs.append(mm_nt(qh, kh) * SCALE)
        grads.append(mm_nt(gh, vh) * live_col)
        at[0, h * T : (h + 1) * T, 0:T] = mm_nt(kh, qh) * SCALE
        at[0, h * T : (h + 1) * T, T : 2 * T] = mm_nt(vh, gh) * live_row
    pairs = jnp.concatenate(pairs, axis=1)
    grads = jnp.concatenate(grads, axis=1)
    head0 = iota(1, (T, HM)) < 64
    grads_high, grads_low = split2(grads)

    def level(y, z, block):
        zs = jnp.concatenate([jnp.where(head0, z, 0.0), jnp.where(head0, 0.0, z)], axis=0)
        zs_high, zs_low = split2(zs)
        same = same_block(block, T, 2 * T)
        score = jnp.dot(jnp.where(same, pairs, 0.0), zs, precision=lax.Precision.HIGHEST, preferred_element_type=F32)
        gh = jnp.where(same, grads_high.astype(F32), 0.0).astype(BF16)
        gl = jnp.where(same, grads_low.astype(F32), 0.0).astype(BF16)
        grad = mm(gh, zs_high) + mm(gl, zs_high) + mm(gh, zs_low)
        if y is None:
            return score, grad
        return y * score, y * grad

    s1, t1 = level(None, inflow, 1)
    for n, size in enumerate(LEVELS):
        start = jnp.bitwise_and(row, -size)
        odd = jnp.bitwise_and(row, size) != 0
        low = jnp.where(odd, start, row + 1)
        high = jnp.where(odd, row, start + size - 1)
        decay = jnp.exp(mask_matmul(one_where((col >= low) & (col <= high)), log_keep))
        yz[0, n] = decay
        odd = odd_half(size)
        score, grad = level(jnp.where(odd, decay, 0.0), jnp.where(odd, 0.0, decay * inflow), 2 * size)
        s1 = s1 + score
        t1 = t1 + grad
    vec[0, 4] = s1
    vec[0, 5] = t1


def second_kernel(turn, place, adv, vec, at, yz, hid, q, og, anchors, *refs):
    core, x, z, y = place[0], place[1], place[2], place[3]
    prompt = jnp.bitwise_xor(core, turn)
    length = place[6 + prompt]
    weight = adv[prompt]
    hid_here, sem = refs[-2:]
    fetch = pltpu.make_async_copy(hid.at[prompt], hid_here, sem)
    fetch.start()
    if turn == 0:
        pd, dgl, kz_out, acc, bacc, kv = refs[:-2]
    else:
        acc_in, bacc_in, pd, dgl, kz_out, dw_keep, dw_send, acc, kv = refs[:-2]
    for i in range(4):
        for j in range(4):
            kv[i, j * 16 : (j + 1) * 16, :] = anchors[jnp.bitwise_xor(x, i), jnp.bitwise_xor(z, j)]

    live_col = jnp.where(iota(0, (T, 1)) < length, weight, 0.0)
    carried = vec[0, 0]
    inflow = vec[0, 1]
    keep = vec[0, 2]
    slope = vec[0, 3]
    head0 = iota(1, (T, HM)) < 64
    anchor_score, anchor_grad = [], []
    for h in range(2):
        cols = slice(h * DH, (h + 1) * DH)
        qh, gh = q[0, :, cols], og[0, :, cols]
        a, b, c = split3(kv[h])
        kz_out[h * 64 : (h + 1) * 64, :] = a
        anchor_score.append(mm_nt(qh, a) + mm_nt(qh, b) + mm_nt(qh, c))
        a, b = split2(kv[2 + h])
        anchor_grad.append(mm_nt(gh, a) + mm_nt(gh, b))
    anchor_score = jnp.concatenate(anchor_score, axis=1) * SCALE
    anchor_grad = jnp.concatenate(anchor_grad, axis=1) * live_col
    scores = vec[0, 4] + carried * anchor_score
    top0 = jnp.max(jnp.where(head0, scores, -jnp.inf), axis=1, keepdims=True)
    top1 = jnp.max(jnp.where(head0, -jnp.inf, scores), axis=1, keepdims=True)
    e = jnp.exp(scores - jnp.where(head0, top0, top1))
    sum0 = jnp.sum(jnp.where(head0, e, 0.0), axis=1, keepdims=True)
    sum1 = jnp.sum(jnp.where(head0, 0.0, e), axis=1, keepdims=True)
    probs = e / jnp.where(head0, sum0, sum1)
    d_probs = vec[0, 5] + carried * anchor_grad
    weighted = probs * d_probs
    dot0 = jnp.sum(jnp.where(head0, weighted, 0.0), axis=1, keepdims=True)
    dot1 = jnp.sum(jnp.where(head0, 0.0, weighted), axis=1, keepdims=True)
    d_scores = probs * (d_probs - jnp.where(head0, dot0, dot1))
    pd[0] = probs
    pd[1] = d_scores

    at_high, at_low = split2(at[0])
    at_high, at_low = at_high.astype(F32), at_low.astype(F32)

    def level(left, block):
        high, low = split2(left)
        same = same_block(block, 2 * T, 2 * T)
        ah = jnp.where(same, at_high, 0.0).astype(BF16)
        al = jnp.where(same, at_low, 0.0).astype(BF16)
        out = mm(ah, high) + mm(al, high) + mm(ah, low)
        return jnp.where(head0, out[0:T], out[T : 2 * T])

    both = jnp.concatenate([d_scores, probs], axis=0)
    held = level(both, 1)
    for n, size in enumerate(LEVELS):
        decay = yz[0, n]
        odd = odd_half(size)
        later = jnp.where(odd, decay, 0.0)
        earlier = jnp.where(odd, 0.0, decay)
        held = held + earlier * level(both * jnp.concatenate([later, later], axis=0), 2 * size)
    change = d_scores * scores + probs * d_probs - held * inflow
    row = iota(0, (T, T))
    col = iota(1, (T, T))
    d_log_keep = mask_matmul(one_where(col >= row), change) - held * keep
    d_gates = d_log_keep * slope
    low_gates = d_gates.astype(BF16)
    dgl[...] = low_gates
    bias = jnp.sum(d_gates, axis=0, keepdims=True)

    fetch.wait()
    update = mm_tn(hid_here[...], low_gates)
    if turn == 0:
        acc[...] = update
        bacc[...] = jnp.broadcast_to(bias, (BROWS, HM))
        return
    acc[...] = acc_in[...] + update
    total = bacc_in[...] + bias
    for kc, out in ((0, dw_keep), (1, dw_send)):
        out[WROWS : WROWS + BROWS, :] = total
        for ky in range(4):
            for kx in range(4):
                block = jnp.bitwise_xor(core, kc) * 16 + jnp.bitwise_xor(y, ky) * 4 + jnp.bitwise_xor(x, kx)
                start = (ky * 4 + kx) * 80
                out[start : start + 80, :] = acc[pl.ds(pl.multiple_of(block * 80, 8), 80), :]


def state_kernel(place, adv, vec_a, vec_b, pd_a, pd_b, q, og, ds_keep, ds_send):
    core, x, z = place[0], place[1], place[2]
    order = iota(0, (HM, HM))
    slot = iota(1, (HM, HM))
    place_c = jnp.bitwise_xor(jnp.bitwise_and(jnp.right_shift(order, 6), 1), core)
    place_x = jnp.bitwise_xor(jnp.bitwise_and(jnp.right_shift(order, 4), 3), x)
    place_z = jnp.bitwise_xor(jnp.bitwise_and(jnp.right_shift(order, 2), 3), z)
    head = jnp.bitwise_and(jnp.right_shift(order, 1), 1)
    wanted = head * 64 + place_z * 16 + place_x * 4 + place_c * 2 + jnp.bitwise_and(order, 1)
    move = one_where(slot == wanted)
    first_head = head == 0
    for turn, vec, pd in ((0, vec_a, pd_a), (1, vec_b, pd_b)):
        prompt = jnp.bitwise_xor(core, turn)
        live_col = jnp.where(iota(0, (T, 1)) < place[6 + prompt], adv[prompt], 0.0)
        carried = vec[0, 0]
        for kind, term in enumerate((pd[1] * carried * SCALE, pd[0] * carried * live_col)):
            data = (q, og)[kind]
            total = 0.0
            for part in split2(term):
                moved = mm_nt(move, part)
                for h in range(2):
                    left = jnp.where(first_head, moved, 0.0) if h == 0 else jnp.where(first_head, 0.0, moved)
                    total = total + mm(left.astype(BF16), data[prompt, :, h * DH : (h + 1) * DH])
            rows = slice(kind * 4, kind * 4 + 4)
            for kc, out in ((0, ds_keep), (1, ds_send)):
                for kx in range(4):
                    for kz in range(4):
                        start = kc * 64 + kx * 16 + kz * 4
                        for lane in range(5):
                            out[kx, kz, prompt, lane, rows, :] = total[start : start + 4, lane * 128 : lane * 128 + 128]


def third_kernel(turn, place, adv, vec, yz, pd, dgl, k0, q, k, og, wg, *refs):
    dq, dk, dv, dx = refs[-4:]
    prompt = jnp.bitwise_xor(place[0], turn)
    length = place[6 + prompt]
    weight = adv[prompt]
    live_col = jnp.where(iota(0, (T, 1)) < length, weight, 0.0)
    dx[0] = mm_nt(dgl[...], wg[...]).astype(BF16)
    inflow = vec[0, 1]
    probs = pd[0]
    d_scores = pd[1]
    head0 = iota(1, (T, HM)) < 64
    both = jnp.concatenate([probs, d_scores], axis=0)

    def level(left, right, block):
        zs = jnp.concatenate([jnp.where(head0, right, 0.0), jnp.where(head0, 0.0, right)], axis=0)
        zh, zl = split2(zs)
        lh, ll = split2(left)
        out = mm_nt(lh, zh) + mm_nt(ll, zh) + mm_nt(lh, zl)
        return jnp.where(same_block(block, 2 * T, 2 * T), out, 0.0)

    mix = level(both, inflow, 1)
    for n, size in enumerate(LEVELS):
        decay = yz[0, n]
        odd = odd_half(size)
        later = jnp.where(odd, decay, 0.0)
        earlier = jnp.where(odd, 0.0, decay * inflow)
        mix = mix + level(both * jnp.concatenate([later, later], axis=0), earlier, 2 * size)
    d_anchor = (d_scores * vec[0, 0]).astype(BF16)
    for h in range(2):
        cols = slice(h * DH, (h + 1) * DH)
        qh, kh, gh = q[0, :, cols], k[0, :, cols], og[0, :, cols]
        mixing = mix[0:T, h * T : (h + 1) * T].astype(BF16).astype(F32)
        d_pairs = mix[T : 2 * T, h * T : (h + 1) * T].astype(BF16)
        from_anchor = mm(d_anchor[:, h * 64 : (h + 1) * 64], k0[h * 64 : (h + 1) * 64, :])
        dq[0, :, cols] = ((mm(d_pairs, kh) + from_anchor) * SCALE).astype(BF16)
        dk[0, :, cols] = (mm_tn(d_pairs, qh) * SCALE).astype(BF16)
        dv[0, :, cols] = mm_tn((mixing * live_col).astype(BF16), gh).astype(BF16)


def place_kernel(half, source, *refs):
    out, sem = refs[-2:]
    core, x, y = lax.axis_index("c"), lax.axis_index("x"), lax.axis_index("y")
    copies = []
    for ky in range(4):
        for kx in range(4):
            block = jnp.bitwise_xor(core, half) * 16 + jnp.bitwise_xor(y, ky) * 4 + jnp.bitwise_xor(x, kx)
            here = out.at[pl.ds(pl.multiple_of(block * 80, 8), 80), :]
            copies.append(pltpu.make_async_copy(source.at[ky, kx], here, sem.at[ky, kx]))
            copies[-1].start()
    for copy in copies:
        copy.wait()


SMEM = pltpu.SMEM
VMEM = pltpu.VMEM


def whole(memory=VMEM):
    return pl.BlockSpec(memory_space=memory)


def fixed(shape):
    return pl.BlockSpec(shape, lambda i, *_: (0,) * len(shape))


def of_prompt(turn, shape):
    return pl.BlockSpec((1,) + shape, lambda i, place, *_: (jnp.bitwise_xor(place[0], turn),) + (0,) * len(shape))


def swap(value, axis, mask):
    count = 1
    for name in axis if isinstance(axis, tuple) else (axis,):
        count *= lax.axis_size(name)
    return lax.ppermute(value, axis, [(i, i ^ mask) for i in range(count)])


def exchange(values, axis):
    out = [values[0]]
    for i in (1, 2, 3):
        out.append(swap(values[i], axis, i))
    return out


def tree_sum(parts):
    while len(parts) > 1:
        parts = [parts[i] + parts[i + 1] for i in range(0, len(parts), 2)]
    return parts[0]


def struct(shape, dtype=F32):
    return jax.ShapeDtypeStruct(shape, dtype)


LIMIT = pltpu.CompilerParams(vmem_limit_bytes=24 * 1024 * 1024)


def local(value):
    return pltpu.with_memory_space_constraint(value, VMEM)


def call(kernel, in_specs, out_specs, out_shape, args, flops, aliases=None, scratch=()):
    return pl.pallas_call(
        kernel,
        grid_spec=pltpu.PrefetchScalarGridSpec(
            num_scalar_prefetch=2, grid=(1,), in_specs=in_specs, out_specs=out_specs, scratch_shapes=scratch
        ),
        out_shape=out_shape,
        input_output_aliases=aliases or {},
        cost_estimate=pl.CostEstimate(flops=int(flops), bytes_accessed=int(3e6), transcendentals=0),
        compiler_params=LIMIT,
    )(*args)


def program(hid, q, k, v, og, wg, bias, prompt_state, owners, lengths, advantage):
    hid, q, k, v, og = (a.reshape(2, T, a.shape[-1]) for a in (hid, q, k, v, og))
    states = prompt_state.reshape(2, 4, 64, DH)
    bias = bias.reshape(1, HM)
    core, x, z, y = (lax.axis_index(n) for n in ("c", "x", "z", "y"))
    zero = jnp.zeros((2,), jnp.int32)
    place = jnp.concatenate([jnp.stack([core, x, z, y]).astype(jnp.int32), zero, lengths.reshape(2)])
    adv = advantage.reshape(2)
    wide = (T, 2 * DH)

    keep, send = pl.pallas_call(
        pick_kernel,
        out_shape=(VMEM((4, 4, 16, DH), F32), VMEM((4, 4, 16, DH), F32)),
        in_specs=[whole(SMEM), whole(pl.ANY)],
        out_specs=(whole(), whole()),
        scratch_shapes=[VMEM((2, 4, 64, DH), F32), pltpu.SemaphoreType.DMA((2,))],
        compiler_params=LIMIT,
        name="pick",
    )(owners, states)

    other = swap(send, "c", 1)
    held = keep + other
    held = tree_sum(exchange([held[i] for i in range(4)], "x"))
    piece = tree_sum(exchange([held[i] for i in range(4)], "z"))
    column = jnp.stack(exchange([piece] * 4, "z"))
    mine = jnp.stack(exchange([column] * 4, "x"))
    other = swap(mine, "c", 1)

    def first(turn):
        return call(
            functools.partial(first_kernel, turn),
            [of_prompt(turn, (T, D))] + [of_prompt(turn, wide)] * 4 + [fixed((D, HM)), fixed((1, HM))],
            (whole(),) * 3,
            (VMEM((1, 6, T, HM), F32), VMEM((1, 2 * T, 2 * T), F32), VMEM((1, 7, T, HM), F32)),
            (place, adv, hid, q, k, v, og, wg, bias),
            3e9,
        )

    def second(turn, early, anchors, extra):
        kv = VMEM((4, 64, DH), F32)
        shapes = (VMEM((2, T, HM), F32), VMEM((T, HM), BF16), VMEM((HM, DH), BF16))
        if turn == 0:
            shapes += (VMEM((D, HM), F32), VMEM((BROWS, HM), F32))
            scratch = [kv]
        else:
            shapes += (VMEM((WROWS + BROWS, HM), F32),) * 2
            scratch = [VMEM((D, HM), F32), kv]
        return call(
            functools.partial(second_kernel, turn),
            [whole()] * 3
            + [whole(pl.ANY), of_prompt(turn, wide), of_prompt(turn, wide), whole()]
            + [whole()] * len(extra),
            (whole(),) * 5,
            shapes,
            (place, adv) + early + (hid, q, og, local(anchors)) + extra,
            3e9,
            scratch=scratch + [VMEM((T, D), BF16), pltpu.SemaphoreType.DMA],
        )

    early_a = tuple(local(a) for a in first(0))
    early_b = tuple(local(a) for a in first(1))
    pd_a, dgl_a, k0_a, acc, bacc = (local(a) for a in second(0, early_a, mine, ()))
    pd_b, dgl_b, k0_b, dw_keep, dw_send = second(1, early_b, other, (acc, bacc))
    pd_b, dgl_b, k0_b = local(pd_b), local(dgl_b), local(k0_b)

    ds_shape = (4, 4, 2, 5, 8, 128)
    ds_keep, ds_send = call(
        state_kernel,
        [whole()] * 4 + [fixed((2,) + wide), fixed((2,) + wide)],
        (whole(),) * 2,
        (VMEM(ds_shape, F32),) * 2,
        (place, adv, early_a[0], early_b[0], pd_a, pd_b, q, og),
        1e9,
    )

    other = swap(dw_send, "c", 1)
    held = dw_keep + other
    tail = held[1280:]
    held = tree_sum(exchange([jnp.concatenate([held[i * 320 : i * 320 + 320], tail]) for i in range(4)], "y"))
    tail = held[320:]
    arrived = swap(ds_send, "c", 1)
    states = (ds_keep + arrived).reshape(4, 320, 128)
    held = tree_sum(exchange([jnp.concatenate([held[i * 80 : i * 80 + 80], tail, states[i]]) for i in range(4)], "x"))
    tail = held[:88]
    held = tree_sum(exchange([jnp.concatenate([tail, held[88 + i * 80 : 168 + i * 80]]) for i in range(4)], "z"))
    d_state = held[88:].reshape(2, 5, 2, 2, 2, 128).transpose(0, 2, 3, 4, 1, 5).reshape(2, 2, 2, 2, DH)
    held = held[:88]
    held = held + swap(held, ("z", "zh"), 7)
    d_bias = held[80]
    piece = held[:80]
    line = jnp.stack(exchange([piece] * 4, "x"))
    mine = jnp.stack(exchange([line] * 4, "y"))
    other = swap(mine, "c", 1)

    def third(turn, early, pd, dgl, k0, earlier):
        return call(
            functools.partial(third_kernel, turn),
            [whole()] * 5
            + [of_prompt(turn, wide)] * 3
            + [fixed((D, HM))]
            + [whole(pl.ANY)] * len(earlier),
            (of_prompt(turn, wide),) * 3 + (of_prompt(turn, (T, D)),),
            (struct((2,) + wide, BF16),) * 3 + (struct((2, T, D), BF16),),
            (place, adv, early[0], early[2], pd, dgl, k0, q, k, og, wg) + earlier,
            3e9,
            aliases={11 + i: i for i in range(len(earlier))},
        )

    outs = third(0, early_a, pd_a, dgl_a, k0_a, ())
    outs = third(1, early_b, pd_b, dgl_b, k0_b, tuple(outs))

    def put(half, source, earlier):
        return pl.pallas_call(
            functools.partial(place_kernel, half),
            out_shape=struct((D, HM)),
            in_specs=[whole()] + [whole(pl.ANY)] * len(earlier),
            out_specs=whole(pl.ANY),
            input_output_aliases={1: 0} if earlier else {},
            scratch_shapes=[pltpu.SemaphoreType.DMA((4, 4))],
            compiler_params=LIMIT,
        )(local(source), *earlier)

    d_weight = put(1, other, (put(0, mine, ()),))

    dq, dk, dv, dx = (a.reshape(1, 2, 1, T, a.shape[-1]) for a in outs)
    return dq, dk, dv, dx, d_weight, d_bias, d_state[None]


def solution(mesh):
    fine = Mesh(mesh.devices.reshape(4, 4, 2, 4, 2), ("z", "x", "c", "y", "zh"))
    comp = ("z", "x", "c")
    rows = ("y", "zh")
    tokens = P(rows, None, comp, None, None)
    return jax.shard_map(
        program,
        mesh=fine,
        in_specs=(tokens,) * 5
        + (P(), P(), P(rows, comp, None, None, None, None, None), P(rows, None), P(rows, None, comp), P(rows, None, comp)),
        out_specs=(tokens,) * 4 + (P(), P(), P(rows, None, None, None, comp, None)),
        check_vma=False,
    )
```

```python
import functools

import jax
import jax.numpy as jnp
from jax import lax
from jax.experimental import pallas as pl
from jax.experimental.pallas import tpu as pltpu
from jax.sharding import Mesh
from jax.sharding import PartitionSpec as P


F32 = jnp.float32
BF16 = jnp.bfloat16
D = 2560
T = 128
HM = 128
DH = 640
LEVELS = (64, 32, 16, 8, 4, 2, 1)
SCALE = DH ** (-0.5)
WROWS = 1280
BROWS = 8


def split2(x):
    high = x.astype(BF16)
    return high, (x - high.astype(F32)).astype(BF16)


def split3(x):
    high = x.astype(BF16)
    rest = x - high.astype(F32)
    middle = rest.astype(BF16)
    return high, middle, (rest - middle.astype(F32)).astype(BF16)


def mm(a, b):
    return jnp.dot(a, b, preferred_element_type=F32)


def mm_nt(a, b):
    return lax.dot_general(a, b, (((1,), (1,)), ((), ())), preferred_element_type=F32)


def mm_tn(a, b):
    return lax.dot_general(a, b, (((0,), (0,)), ((), ())), preferred_element_type=F32)


def mask_matmul(mask, x):
    high, middle, low = split3(x)
    return mm(mask, high) + mm(mask, middle) + mm(mask, low)


def iota(dim, shape):
    return lax.broadcasted_iota(jnp.int32, shape, dim)


def one_where(condition):
    return jnp.where(condition, 1.0, 0.0).astype(BF16)


def same_block(size, rows, cols):
    shift = size.bit_length() - 1
    row = jnp.right_shift(jnp.bitwise_and(iota(0, (rows, cols)), T - 1), shift)
    col = jnp.right_shift(jnp.bitwise_and(iota(1, (rows, cols)), T - 1), shift)
    return row == col


def odd_half(size):
    return jnp.bitwise_and(iota(0, (T, HM)), size) != 0


def pick_kernel(owners, states, keep, send, sems):
    core, x, z = lax.axis_index("c"), lax.axis_index("x"), lax.axis_index("z")
    index = (z * 4 + x) * 2 + core

    def copies(turn, out):
        prompt = jnp.bitwise_xor(core, turn)
        for kx in range(4):
            for kz in range(4):
                row = pl.multiple_of(jnp.bitwise_xor(z, kz) * 16, 16)
                source = states.at[prompt, jnp.bitwise_xor(x, kx), pl.ds(row, 16), :]
                yield pltpu.make_async_copy(source, out.at[kx, kz], sems.at[turn, kx, kz])

    for step in ("start", "wait"):
        for turn, out in ((1, send), (0, keep)):
            owned = owners[0, jnp.bitwise_xor(core, turn)] == index

            @pl.when(owned)
            def _():
                for copy in copies(turn, out):
                    getattr(copy, step)()

            if step == "start":

                @pl.when(jnp.logical_not(owned))
                def _():
                    out[...] = jnp.zeros_like(out)


def first_kernel(turn, place, adv, hid, q, k, v, og, wg, bias, vec, at, yz):
    prompt = jnp.bitwise_xor(place[0], turn)
    length = place[6 + prompt]
    weight = adv[prompt]
    gates = mm(hid[0], wg[...]) + bias[...]
    u = jnp.exp(-jnp.abs(gates))
    s = u / (2.0 + u)
    s2 = s * s
    series = 1.0 / 17.0
    for n in (15, 13, 11, 9, 7, 5, 3, 1):
        series = series * s2 + 1.0 / n
    log1p = 2.0 * s * series
    log_keep = (jnp.minimum(gates, 0.0) - log1p) * 0.125
    keep = jnp.exp(log_keep)
    near = 1.0 + log_keep * (1.0 / 8.0)
    for n in (7, 6, 5, 4, 3, 2):
        near = 1.0 + log_keep * (1.0 / n) * near
    inflow = jnp.where(log_keep > -0.3, -log_keep * near, 1.0 - keep)
    slope = jnp.where(gates >= 0.0, u, 1.0) / (1.0 + u) * 0.125
    row = iota(0, (T, T))
    col = iota(1, (T, T))
    running = mask_matmul(one_where(col <= row), log_keep)
    vec[0, 0] = jnp.exp(running)
    vec[0, 1] = inflow
    vec[0, 2] = keep
    vec[0, 3] = slope

    live_col = jnp.where(iota(0, (T, 1)) < length, weight, 0.0)
    live_row = jnp.where(iota(1, (1, T)) < length, weight, 0.0)
    pairs, grads = [], []
    for h in range(2):
        cols = slice(h * DH, (h + 1) * DH)
        qh, kh, vh, gh = q[0, :, cols], k[0, :, cols], v[0, :, cols], og[0, :, cols]
        pairs.append(mm_nt(qh, kh) * SCALE)
        grads.append(mm_nt(gh, vh) * live_col)
        at[0, h * T : (h + 1) * T, 0:T] = mm_nt(kh, qh) * SCALE
        at[0, h * T : (h + 1) * T, T : 2 * T] = mm_nt(vh, gh) * live_row
    pairs = jnp.concatenate(pairs, axis=1)
    grads = jnp.concatenate(grads, axis=1)
    head0 = iota(1, (T, HM)) < 64
    grads_high, grads_low = split2(grads)

    def level(y, z, block):
        zs = jnp.concatenate([jnp.where(head0, z, 0.0), jnp.where(head0, 0.0, z)], axis=0)
        zs_high, zs_low = split2(zs)
        same = same_block(block, T, 2 * T)
        score = jnp.dot(jnp.where(same, pairs, 0.0), zs, precision=lax.Precision.HIGHEST, preferred_element_type=F32)
        gh = jnp.where(same, grads_high.astype(F32), 0.0).astype(BF16)
        gl = jnp.where(same, grads_low.astype(F32), 0.0).astype(BF16)
        grad = mm(gh, zs_high) + mm(gl, zs_high) + mm(gh, zs_low)
        if y is None:
            return score, grad
        return y * score, y * grad

    s1, t1 = level(None, inflow, 1)
    for n, size in enumerate(LEVELS):
        start = jnp.bitwise_and(row, -size)
        odd = jnp.bitwise_and(row, size) != 0
        low = jnp.where(odd, start, row + 1)
        high = jnp.where(odd, row, start + size - 1)
        decay = jnp.exp(mask_matmul(one_where((col >= low) & (col <= high)), log_keep))
        yz[0, n] = decay
        odd = odd_half(size)
        score, grad = level(jnp.where(odd, decay, 0.0), jnp.where(odd, 0.0, decay * inflow), 2 * size)
        s1 = s1 + score
        t1 = t1 + grad
    vec[0, 4] = s1
    vec[0, 5] = t1


def second_kernel(turn, place, adv, vec, at, yz, hid, q, og, anchors, *refs):
    core, x, z, y = place[0], place[1], place[2], place[3]
    prompt = jnp.bitwise_xor(core, turn)
    length = place[6 + prompt]
    weight = adv[prompt]
    hid_here, sem = refs[-2:]
    fetch = pltpu.make_async_copy(hid.at[prompt], hid_here, sem)
    fetch.start()
    if turn == 0:
        pd, dgl, kz_out, acc, bacc, kv = refs[:-2]
    else:
        acc_in, bacc_in, pd, dgl, kz_out, dw_keep, dw_send, acc, kv = refs[:-2]
    for i in range(4):
        for j in range(4):
            kv[i, j * 16 : (j + 1) * 16, :] = anchors[jnp.bitwise_xor(x, i), jnp.bitwise_xor(z, j)]

    live_col = jnp.where(iota(0, (T, 1)) < length, weight, 0.0)
    carried = vec[0, 0]
    inflow = vec[0, 1]
    keep = vec[0, 2]
    slope = vec[0, 3]
    head0 = iota(1, (T, HM)) < 64
    anchor_score, anchor_grad = [], []
    for h in range(2):
        cols = slice(h * DH, (h + 1) * DH)
        qh, gh = q[0, :, cols], og[0, :, cols]
        a, b, c = split3(kv[h])
        kz_out[h * 64 : (h + 1) * 64, :] = a
        anchor_score.append(mm_nt(qh, a) + mm_nt(qh, b) + mm_nt(qh, c))
        a, b = split2(kv[2 + h])
        anchor_grad.append(mm_nt(gh, a) + mm_nt(gh, b))
    anchor_score = jnp.concatenate(anchor_score, axis=1) * SCALE
    anchor_grad = jnp.concatenate(anchor_grad, axis=1) * live_col
    scores = vec[0, 4] + carried * anchor_score
    top0 = jnp.max(jnp.where(head0, scores, -jnp.inf), axis=1, keepdims=True)
    top1 = jnp.max(jnp.where(head0, -jnp.inf, scores), axis=1, keepdims=True)
    e = jnp.exp(scores - jnp.where(head0, top0, top1))
    sum0 = jnp.sum(jnp.where(head0, e, 0.0), axis=1, keepdims=True)
    sum1 = jnp.sum(jnp.where(head0, 0.0, e), axis=1, keepdims=True)
    probs = e / jnp.where(head0, sum0, sum1)
    d_probs = vec[0, 5] + carried * anchor_grad
    weighted = probs * d_probs
    dot0 = jnp.sum(jnp.where(head0, weighted, 0.0), axis=1, keepdims=True)
    dot1 = jnp.sum(jnp.where(head0, 0.0, weighted), axis=1, keepdims=True)
    d_scores = probs * (d_probs - jnp.where(head0, dot0, dot1))
    pd[0] = probs
    pd[1] = d_scores

    at_high, at_low = split2(at[0])
    at_high, at_low = at_high.astype(F32), at_low.astype(F32)

    def level(left, block):
        high, low = split2(left)
        same = same_block(block, 2 * T, 2 * T)
        ah = jnp.where(same, at_high, 0.0).astype(BF16)
        al = jnp.where(same, at_low, 0.0).astype(BF16)
        out = mm(ah, high) + mm(al, high) + mm(ah, low)
        return jnp.where(head0, out[0:T], out[T : 2 * T])

    both = jnp.concatenate([d_scores, probs], axis=0)
    held = level(both, 1)
    for n, size in enumerate(LEVELS):
        decay = yz[0, n]
        odd = odd_half(size)
        later = jnp.where(odd, decay, 0.0)
        earlier = jnp.where(odd, 0.0, decay)
        held = held + earlier * level(both * jnp.concatenate([later, later], axis=0), 2 * size)
    change = d_scores * scores + probs * d_probs - held * inflow
    row = iota(0, (T, T))
    col = iota(1, (T, T))
    d_log_keep = mask_matmul(one_where(col >= row), change) - held * keep
    d_gates = d_log_keep * slope
    low_gates = d_gates.astype(BF16)
    dgl[...] = low_gates
    bias = jnp.sum(d_gates, axis=0, keepdims=True)

    fetch.wait()
    update = mm_tn(hid_here[...], low_gates)
    if turn == 0:
        acc[...] = update
        bacc[...] = jnp.broadcast_to(bias, (BROWS, HM))
        return
    acc[...] = acc_in[...] + update
    total = bacc_in[...] + bias
    for kc, out in ((0, dw_keep), (1, dw_send)):
        out[WROWS : WROWS + BROWS, :] = total
        for ky in range(4):
            for kx in range(4):
                block = jnp.bitwise_xor(core, kc) * 16 + jnp.bitwise_xor(y, ky) * 4 + jnp.bitwise_xor(x, kx)
                start = (ky * 4 + kx) * 80
                out[start : start + 80, :] = acc[pl.ds(pl.multiple_of(block * 80, 8), 80), :]


def state_kernel(place, adv, vec_a, vec_b, pd_a, pd_b, q, og, ds_keep, ds_send):
    core, x, z = place[0], place[1], place[2]
    order = iota(0, (HM, HM))
    slot = iota(1, (HM, HM))
    place_c = jnp.bitwise_xor(jnp.bitwise_and(jnp.right_shift(order, 6), 1), core)
    place_x = jnp.bitwise_xor(jnp.bitwise_and(jnp.right_shift(order, 4), 3), x)
    place_z = jnp.bitwise_xor(jnp.bitwise_and(jnp.right_shift(order, 2), 3), z)
    head = jnp.bitwise_and(jnp.right_shift(order, 1), 1)
    wanted = head * 64 + place_z * 16 + place_x * 4 + place_c * 2 + jnp.bitwise_and(order, 1)
    move = one_where(slot == wanted)
    first_head = head == 0
    for turn, vec, pd in ((0, vec_a, pd_a), (1, vec_b, pd_b)):
        prompt = jnp.bitwise_xor(core, turn)
        live_col = jnp.where(iota(0, (T, 1)) < place[6 + prompt], adv[prompt], 0.0)
        carried = vec[0, 0]
        for kind, term in enumerate((pd[1] * carried * SCALE, pd[0] * carried * live_col)):
            data = (q, og)[kind]
            total = 0.0
            for part in split2(term):
                moved = mm_nt(move, part)
                for h in range(2):
                    left = jnp.where(first_head, moved, 0.0) if h == 0 else jnp.where(first_head, 0.0, moved)
                    total = total + mm(left.astype(BF16), data[prompt, :, h * DH : (h + 1) * DH])
            rows = slice(kind * 4, kind * 4 + 4)
            for kc, out in ((0, ds_keep), (1, ds_send)):
                for kx in range(4):
                    for kz in range(4):
                        start = kc * 64 + kx * 16 + kz * 4
                        for lane in range(5):
                            out[kx, kz, prompt, lane, rows, :] = total[start : start + 4, lane * 128 : lane * 128 + 128]


def third_kernel(turn, place, adv, vec, yz, pd, dgl, k0, q, k, og, wg, *refs):
    dq, dk, dv, dx = refs[-4:]
    prompt = jnp.bitwise_xor(place[0], turn)
    length = place[6 + prompt]
    weight = adv[prompt]
    live_col = jnp.where(iota(0, (T, 1)) < length, weight, 0.0)
    dx[0] = mm_nt(dgl[...], wg[...]).astype(BF16)
    inflow = vec[0, 1]
    probs = pd[0]
    d_scores = pd[1]
    head0 = iota(1, (T, HM)) < 64
    both = jnp.concatenate([probs, d_scores], axis=0)

    def level(left, right, block):
        zs = jnp.concatenate([jnp.where(head0, right, 0.0), jnp.where(head0, 0.0, right)], axis=0)
        zh, zl = split2(zs)
        lh, ll = split2(left)
        out = mm_nt(lh, zh) + mm_nt(ll, zh) + mm_nt(lh, zl)
        return jnp.where(same_block(block, 2 * T, 2 * T), out, 0.0)

    mix = level(both, inflow, 1)
    for n, size in enumerate(LEVELS):
        decay = yz[0, n]
        odd = odd_half(size)
        later = jnp.where(odd, decay, 0.0)
        earlier = jnp.where(odd, 0.0, decay * inflow)
        mix = mix + level(both * jnp.concatenate([later, later], axis=0), earlier, 2 * size)
    d_anchor = (d_scores * vec[0, 0]).astype(BF16)
    for h in range(2):
        cols = slice(h * DH, (h + 1) * DH)
        qh, kh, gh = q[0, :, cols], k[0, :, cols], og[0, :, cols]
        mixing = mix[0:T, h * T : (h + 1) * T].astype(BF16).astype(F32)
        d_pairs = mix[T : 2 * T, h * T : (h + 1) * T].astype(BF16)
        from_anchor = mm(d_anchor[:, h * 64 : (h + 1) * 64], k0[h * 64 : (h + 1) * 64, :])
        dq[0, :, cols] = ((mm(d_pairs, kh) + from_anchor) * SCALE).astype(BF16)
        dk[0, :, cols] = (mm_tn(d_pairs, qh) * SCALE).astype(BF16)
        dv[0, :, cols] = mm_tn((mixing * live_col).astype(BF16), gh).astype(BF16)


def place_kernel(half, source, *refs):
    out, sem = refs[-2:]
    core, x, y = lax.axis_index("c"), lax.axis_index("x"), lax.axis_index("y")
    copies = []
    for ky in range(4):
        for kx in range(4):
            block = jnp.bitwise_xor(core, half) * 16 + jnp.bitwise_xor(y, ky) * 4 + jnp.bitwise_xor(x, kx)
            here = out.at[pl.ds(pl.multiple_of(block * 80, 8), 80), :]
            copies.append(pltpu.make_async_copy(source.at[ky, kx], here, sem.at[ky, kx]))
            copies[-1].start()
    for copy in copies:
        copy.wait()


SMEM = pltpu.SMEM
VMEM = pltpu.VMEM


def whole(memory=VMEM):
    return pl.BlockSpec(memory_space=memory)


def fixed(shape):
    return pl.BlockSpec(shape, lambda i, *_: (0,) * len(shape))


def of_prompt(turn, shape):
    return pl.BlockSpec((1,) + shape, lambda i, place, *_: (jnp.bitwise_xor(place[0], turn),) + (0,) * len(shape))


def swap(value, axis, mask):
    count = 1
    for name in axis if isinstance(axis, tuple) else (axis,):
        count *= lax.axis_size(name)
    return lax.ppermute(value, axis, [(i, i ^ mask) for i in range(count)])


def exchange(values, axis):
    out = [values[0]]
    for i in (1, 2, 3):
        out.append(swap(values[i], axis, i))
    return out


def tree_sum(parts):
    while len(parts) > 1:
        parts = [parts[i] + parts[i + 1] for i in range(0, len(parts), 2)]
    return parts[0]


def struct(shape, dtype=F32):
    return jax.ShapeDtypeStruct(shape, dtype)


LIMIT = pltpu.CompilerParams(vmem_limit_bytes=24 * 1024 * 1024)


def local(value):
    return pltpu.with_memory_space_constraint(value, VMEM)


def call(kernel, in_specs, out_specs, out_shape, args, flops, aliases=None, scratch=()):
    return pl.pallas_call(
        kernel,
        grid_spec=pltpu.PrefetchScalarGridSpec(
            num_scalar_prefetch=2, grid=(1,), in_specs=in_specs, out_specs=out_specs, scratch_shapes=scratch
        ),
        out_shape=out_shape,
        input_output_aliases=aliases or {},
        cost_estimate=pl.CostEstimate(flops=int(flops), bytes_accessed=int(3e6), transcendentals=0),
        compiler_params=LIMIT,
    )(*args)


def program(hid, q, k, v, og, wg, bias, prompt_state, owners, lengths, advantage):
    hid, q, k, v, og = (a.reshape(2, T, a.shape[-1]) for a in (hid, q, k, v, og))
    states = prompt_state.reshape(2, 4, 64, DH)
    bias = bias.reshape(1, HM)
    core, x, z, y = (lax.axis_index(n) for n in ("c", "x", "z", "y"))
    zero = jnp.zeros((2,), jnp.int32)
    place = jnp.concatenate([jnp.stack([core, x, z, y]).astype(jnp.int32), zero, lengths.reshape(2)])
    adv = advantage.reshape(2)
    wide = (T, 2 * DH)

    keep, send = pl.pallas_call(
        pick_kernel,
        out_shape=(VMEM((4, 4, 16, DH), F32), VMEM((4, 4, 16, DH), F32)),
        in_specs=[whole(SMEM), whole(pl.ANY)],
        out_specs=(whole(), whole()),
        scratch_shapes=[pltpu.SemaphoreType.DMA((2, 4, 4))],
        compiler_params=LIMIT,
        name="pick",
    )(pltpu.with_memory_space_constraint(owners, pltpu.HBM), pltpu.with_memory_space_constraint(states, pltpu.HBM))

    other = swap(send, "c", 1)
    held = keep + other
    held = tree_sum(exchange([held[i] for i in range(4)], "x"))
    piece = tree_sum(exchange([held[i] for i in range(4)], "z"))
    column = jnp.stack(exchange([piece] * 4, "z"))
    mine = jnp.stack(exchange([column] * 4, "x"))
    other = swap(mine, "c", 1)

    def first(turn):
        return call(
            functools.partial(first_kernel, turn),
            [of_prompt(turn, (T, D))] + [of_prompt(turn, wide)] * 4 + [fixed((D, HM)), fixed((1, HM))],
            (whole(),) * 3,
            (VMEM((1, 6, T, HM), F32), VMEM((1, 2 * T, 2 * T), F32), VMEM((1, 7, T, HM), F32)),
            (place, adv, hid, q, k, v, og, wg, bias),
            3e9,
        )

    def second(turn, early, anchors, extra):
        kv = VMEM((4, 64, DH), F32)
        shapes = (VMEM((2, T, HM), F32), VMEM((T, HM), BF16), VMEM((HM, DH), BF16))
        if turn == 0:
            shapes += (VMEM((D, HM), F32), VMEM((BROWS, HM), F32))
            scratch = [kv]
        else:
            shapes += (VMEM((WROWS + BROWS, HM), F32),) * 2
            scratch = [VMEM((D, HM), F32), kv]
        return call(
            functools.partial(second_kernel, turn),
            [whole()] * 3
            + [whole(pl.ANY), of_prompt(turn, wide), of_prompt(turn, wide), whole()]
            + [whole()] * len(extra),
            (whole(),) * 5,
            shapes,
            (place, adv) + early + (hid, q, og, local(anchors)) + extra,
            3e9,
            scratch=scratch + [VMEM((T, D), BF16), pltpu.SemaphoreType.DMA],
        )

    early_a = tuple(local(a) for a in first(0))
    early_b = tuple(local(a) for a in first(1))
    pd_a, dgl_a, k0_a, acc, bacc = (local(a) for a in second(0, early_a, mine, ()))
    pd_b, dgl_b, k0_b, dw_keep, dw_send = second(1, early_b, other, (acc, bacc))
    pd_b, dgl_b, k0_b = local(pd_b), local(dgl_b), local(k0_b)

    ds_shape = (4, 4, 2, 5, 8, 128)
    ds_keep, ds_send = call(
        state_kernel,
        [whole()] * 4 + [fixed((2,) + wide), fixed((2,) + wide)],
        (whole(),) * 2,
        (VMEM(ds_shape, F32),) * 2,
        (place, adv, early_a[0], early_b[0], pd_a, pd_b, q, og),
        1e9,
    )

    other = swap(dw_send, "c", 1)
    held = dw_keep + other
    tail = held[1280:]
    held = tree_sum(exchange([jnp.concatenate([held[i * 320 : i * 320 + 320], tail]) for i in range(4)], "y"))
    tail = held[320:]
    arrived = swap(ds_send, "c", 1)
    states = (ds_keep + arrived).reshape(4, 320, 128)
    held = tree_sum(exchange([jnp.concatenate([held[i * 80 : i * 80 + 80], tail, states[i]]) for i in range(4)], "x"))
    tail = held[:88]
    held = tree_sum(exchange([jnp.concatenate([tail, held[88 + i * 80 : 168 + i * 80]]) for i in range(4)], "z"))
    d_state = held[88:].reshape(2, 5, 2, 2, 2, 128).transpose(0, 2, 3, 4, 1, 5).reshape(2, 2, 2, 2, DH)
    held = held[:88]
    held = held + swap(held, ("z", "zh"), 7)
    d_bias = held[80]
    piece = held[:80]
    line = jnp.stack(exchange([piece] * 4, "x"))
    mine = jnp.stack(exchange([line] * 4, "y"))
    other = swap(mine, "c", 1)

    def third(turn, early, pd, dgl, k0, earlier):
        return call(
            functools.partial(third_kernel, turn),
            [whole()] * 5
            + [of_prompt(turn, wide)] * 3
            + [fixed((D, HM))]
            + [whole(pl.ANY)] * len(earlier),
            (of_prompt(turn, wide),) * 3 + (of_prompt(turn, (T, D)),),
            (struct((2,) + wide, BF16),) * 3 + (struct((2, T, D), BF16),),
            (place, adv, early[0], early[2], pd, dgl, k0, q, k, og, wg) + earlier,
            3e9,
            aliases={11 + i: i for i in range(len(earlier))},
        )

    outs = third(0, early_a, pd_a, dgl_a, k0_a, ())
    outs = third(1, early_b, pd_b, dgl_b, k0_b, tuple(outs))

    def put(half, source, earlier):
        return pl.pallas_call(
            functools.partial(place_kernel, half),
            out_shape=struct((D, HM)),
            in_specs=[whole()] + [whole(pl.ANY)] * len(earlier),
            out_specs=whole(pl.ANY),
            input_output_aliases={1: 0} if earlier else {},
            scratch_shapes=[pltpu.SemaphoreType.DMA((4, 4))],
            compiler_params=LIMIT,
        )(local(source), *earlier)

    d_weight = put(1, other, (put(0, mine, ()),))

    dq, dk, dv, dx = (a.reshape(1, 2, 1, T, a.shape[-1]) for a in outs)
    return dq, dk, dv, dx, d_weight, d_bias, d_state[None]


def solution(mesh):
    fine = Mesh(mesh.devices.reshape(4, 4, 2, 4, 2), ("z", "x", "c", "y", "zh"))
    comp = ("z", "x", "c")
    rows = ("y", "zh")
    tokens = P(rows, None, comp, None, None)
    return jax.shard_map(
        program,
        mesh=fine,
        in_specs=(tokens,) * 5
        + (P(), P(), P(rows, comp, None, None, None, None, None), P(rows, None), P(rows, None, comp), P(rows, None, comp)),
        out_specs=(tokens,) * 4 + (P(), P(), P(rows, None, None, None, comp, None)),
        check_vma=False,
    )
```
